256 devices in a mesh: frames: 16 (over x_hi, z), rows: 16 (over y, x_lo, core).
Axes of the slice: x: 4 (x_hi: 2, x_lo: 2; x = x_hi * 2 + x_lo), y: 4, z: 8, core: 2. Of those that a mesh axis runs over, the one named last changes fastest.
Arguments:
- video: bfloat16 [32, 32, 128, 256], P('frames', 'rows'), may hold values from -6 to 6
- norm_a: float32 [256], replicated, may hold values from 0.5 to 2
- conv_a: bfloat16 [3, 3, 3, 256, 256], replicated, may hold values from -0.078125 to 0.078125
- norm_b: float32 [256], replicated, may hold values from 0.5 to 2
- conv_b: bfloat16 [3, 3, 3, 256, 256], replicated, may hold values from -0.078125 to 0.078125
- norm_c: float32 [256], replicated, may hold values from 0.5 to 2
- w_query: bfloat16 [256, 256], replicated, may hold values from -2 to 2
- w_key: bfloat16 [256, 256], replicated, may hold values from -2 to 2
- w_value: bfloat16 [256, 256], replicated, may hold values from -0.375 to 0.375
- w_out: bfloat16 [256, 256], replicated, may hold values from -0.375 to 0.375
Outputs:
- encoded: bfloat16 [32, 32, 128, 256], P('frames', 'rows')
The draws below stay inside these ranges and needn't reach their ends.
All inputs are finite; a program needn't handle non-finite values.
Results may differ from the reference program's by a relative error of at most 0.015.
Values may be sent and summed in bfloat16 or wider, within the bound.
A program may use at most 64 MiB of HBM per device.

```python
import math
import jax
import jax.numpy as jnp
from jax import lax

C = 256
HEADS = 8
WIDTH = 128
FRAMES = 32
ROWS = 32


def query_key_pair(key):
    base_key = jax.random.fold_in(key, 4321)
    first, second = jax.random.split(base_key, 2)
    base = jax.random.truncated_normal(first, -3.0, 3.0, (C, C), jnp.float32) * C ** (-0.5)
    other = jax.random.truncated_normal(second, -3.0, 3.0, (C, C), jnp.float32) * C ** (-0.5)
    query = base
    keyed = other
    return (query, keyed)


def draw_w_query(key, part):
    return query_key_pair(key)[0].astype(jnp.bfloat16)


def draw_w_key(key, part):
    return query_key_pair(key)[1].astype(jnp.bfloat16)


def levels(key, extent, shards, low, largest):
    factor_of = 1.0
    for axis_at, blocks in shards:
        draws = jax.random.uniform(jax.random.fold_in(jax.random.fold_in(key, 6), axis_at), (blocks,), jnp.float32, low / len(shards), largest / len(shards))
        factor_of = factor_of * jnp.repeat(jnp.exp(draws), extent[axis_at] // blocks).reshape((-1,) + (1,) * (len(extent) - 1 - axis_at))
    return factor_of


def scatter_about(stream_key, extent, width, bound, cuts=(), kind=jnp.bfloat16):
    entries = width * jax.random.normal(stream_key, extent, jnp.float32)
    if cuts:
        entries = entries * levels(stream_key, extent, cuts, -0.22, 0.18)
    return jnp.clip(entries, -bound, bound).astype(kind)


def setup_inputs(seed: int = 0) -> dict:
    arg_keys = jax.random.split(jax.random.key(seed), 11)
    return {
        "video": scatter_about(arg_keys[0], (FRAMES, ROWS, WIDTH, C), 1.0, 6.0, ((0, 16), (1, 16))),
        "norm_a": jnp.clip(jnp.exp(jax.random.uniform(arg_keys[1], (C,), jnp.float32, math.log(0.5), math.log(2.0))), 0.5, 2.0),
        "conv_a": scatter_about(arg_keys[2], (3, 3, 3, C, C), (27 * C) ** -0.5, 0.078125),
        "norm_b": jnp.clip(jnp.exp(jax.random.uniform(arg_keys[3], (C,), jnp.float32, math.log(0.5), math.log(2.0))), 0.5, 2.0),
        "conv_b": scatter_about(arg_keys[4], (3, 3, 3, C, C), (27 * C) ** -0.5, 0.078125),
        "norm_c": jnp.clip(jnp.exp(jax.random.uniform(arg_keys[5], (C,), jnp.float32, math.log(0.5), math.log(2.0))), 0.5, 2.0),
        "w_query": draw_w_query(jax.random.fold_in(arg_keys[10], 71), 0),
        "w_key": draw_w_key(jax.random.fold_in(arg_keys[10], 71), 0),
        "w_value": scatter_about(arg_keys[8], (C, C), C ** -0.5, 0.375),
        "w_out": scatter_about(arg_keys[9], (C, C), C ** -0.5, 0.375),
    }


def norm_scale(values, gain):
    floats = values.astype(jnp.float32)
    mean_sq = lax.optimization_barrier(jnp.mean(floats * floats, axis=-1, keepdims=True))
    return floats * lax.rsqrt(mean_sq + 1e-06) * gain

def causal_conv(active, kernel):
    frames_all, rows_all, width_all, channels = active.shape
    padded = jnp.pad(active, ((2, 0), (1, 1), (1, 1), (0, 0)))
    total = jnp.zeros((frames_all * rows_all * width_all, kernel.shape[-1]), jnp.float32)
    for lag_time in range(3):
        for row_step in range(3):
            for col_step in range(3):
                slab = padded[lag_time:lag_time + frames_all, row_step:row_step + rows_all, col_step:col_step + width_all]
                total = total + jnp.dot(slab.reshape(-1, channels), kernel[lag_time, row_step, col_step], preferred_element_type=jnp.float32)
    return total.reshape(frames_all, rows_all, width_all, -1)

def reference(video, norm_a, conv_a, norm_b, conv_b, norm_c, w_query, w_key, w_value, w_out):
    act_a = jax.nn.silu(norm_scale(video, norm_a)).astype(jnp.bfloat16)
    inner = causal_conv(act_a, conv_a).astype(jnp.bfloat16)
    act_b = jax.nn.silu(norm_scale(inner, norm_b)).astype(jnp.bfloat16)
    block = (video.astype(jnp.float32) + causal_conv(act_b, conv_b)).astype(jnp.bfloat16)
    normed = norm_scale(block, norm_c).astype(jnp.bfloat16)
    frames_all, rows_all, width_all, channels = block.shape
    head_dim = channels // HEADS
    query = jnp.dot(normed, w_query, preferred_element_type=jnp.float32).astype(jnp.bfloat16)
    keyed = jnp.dot(normed, w_key, preferred_element_type=jnp.float32).astype(jnp.bfloat16)
    valued = jnp.dot(normed, w_value, preferred_element_type=jnp.float32).astype(jnp.bfloat16)
    shape4 = (frames_all, rows_all * width_all, HEADS, head_dim)
    query = query.reshape(shape4).astype(jnp.float32)
    keyed = keyed.reshape(shape4).astype(jnp.float32)
    valued = valued.reshape(shape4).astype(jnp.float32)
    scores = jnp.einsum('tphd,sphd->phts', query, keyed) * head_dim ** (-0.5)
    later = lax.broadcasted_iota(jnp.int32, (frames_all, frames_all), 0)
    earlier = lax.broadcasted_iota(jnp.int32, (frames_all, frames_all), 1)
    scores = jnp.where(later >= earlier, scores, -1e+30)
    top = lax.optimization_barrier(jnp.max(scores, axis=-1, keepdims=True))
    expd = jnp.exp(scores - top)
    probs = (expd / lax.optimization_barrier(jnp.sum(expd, axis=-1, keepdims=True))).astype(jnp.bfloat16)
    attended = jnp.einsum('phts,sphd->tphd', probs.astype(jnp.float32), valued).astype(jnp.bfloat16)
    attended = attended.reshape(frames_all, rows_all, width_all, channels)
    projected = jnp.dot(attended, w_out, preferred_element_type=jnp.float32).astype(jnp.bfloat16)
    return (block.astype(jnp.float32) + projected.astype(jnp.float32)).astype(jnp.bfloat16)
```

```python
import functools

import jax
import jax.numpy as jnp
from jax import lax
from jax.experimental import pallas as pl
from jax.experimental.pallas import tpu as pltpu
from jax.sharding import PartitionSpec as P

MESH = pl.DeviceIdType.MESH
HEADS = 8
C = 256
T = 32
F = 16
R = 16
PATCH = 8
BF = jnp.bfloat16
F32 = jnp.float32


def snake(i):
    half = i // 8
    return i + half * (23 - 2 * i)


def rms(x, gain):
    ms = jnp.mean(x * x, axis=-1, keepdims=True)
    return x * lax.rsqrt(ms + 1e-06) * gain


def silu(x):
    h = 0.5 * x
    return h + h * jnp.tanh(h)


def dot(a, b):
    return jnp.dot(a, b, preferred_element_type=F32)


def dot_tt(a, b, dims):
    return lax.dot_general(a, b, (dims, ((), ())), preferred_element_type=F32)


def shift_rows(y, by):
    rolled = pltpu.roll(y, by, 0)
    frame = lax.broadcasted_iota(jnp.int32, y.shape, 0) % T
    return jnp.where(frame >= by, rolled, 0.0)


def conv_rows(act, kern, row):
    parts = []
    for i in range(3):
        total = None
        for j in range(3):
            for l in range(3):
                slab = act[row + j, l : l + PATCH].reshape(PATCH * T, C)
                term = dot(slab, kern[i * 9 + j * 3 + l])
                total = term if total is None else total + term
        parts.append(total)
    return parts[2] + shift_rows(parts[1], 1) + shift_rows(parts[0], 2)


def one_hot(rows_to):
    a = lax.broadcasted_iota(jnp.int32, (512, 512), 0)
    b = lax.broadcasted_iota(jnp.int32, (512, 512), 1)
    return jnp.where(b == rows_to(a), 1.0, 0.0).astype(BF)


def attend_pixel(q, k, v):
    halves = []
    lane_head = lax.broadcasted_iota(jnp.int32, (T, 128), 1) // 32
    s_at = lax.broadcasted_iota(jnp.int32, (T, 128), 0)
    t_at = lax.broadcasted_iota(jnp.int32, (T, 128), 1) % 32
    for hh in range(2):
        lanes = slice(128 * hh, 128 * hh + 128)
        qh, kh, vh = q[:, lanes], k[:, lanes], v[:, lanes]
        blocks = [jnp.where(lane_head == h, qh.astype(F32), 0.0).astype(BF) for h in range(4)]
        q_bd = jnp.concatenate(blocks, axis=0)
        s = dot_tt(kh, q_bd, ((1,), (1,))) * (32 ** -0.5)
        s = jnp.where(s_at <= t_at, s, -1e30)
        e = jnp.exp(s - jnp.max(s, axis=0, keepdims=True))
        p = (e / jnp.sum(e, axis=0, keepdims=True)).astype(BF)
        o = dot_tt(p, vh, ((0,), (0,)))
        att = jnp.zeros((T, 128), F32)
        for h in range(4):
            att = jnp.where(lane_head == h, o[32 * h : 32 * h + 32], att)
        halves.append(att.astype(BF))
    return halves


def kernel(video, na, ca, nb, cb, nc, wq, wk, wv, wo, out,
           vloc, rin, xres, act_a, act_b, ka, kb, ga, gb, gc, sq, sk, sv, so,
           fwd, bwd, qs, ks, vs, att, blk, sbuf,
           lsem, in_send, in_recv, ha_send, ha_recv, hb_send, hb_recv, out_send, out_recv):
    f = lax.axis_index("frames")
    r = lax.axis_index("rows")
    g = snake(f)
    up, down = (r + R - 1) % R, (r + 1) % R
    west, east = snake((g + F - 1) % F), snake((g + 1) % F)

    loads = [pltpu.make_async_copy(src, dst, lsem.at[n]) for n, (src, dst) in enumerate(
        [(video, vloc), (na, ga), (ca, ka), (nb, gb), (cb, kb), (nc, gc),
         (wq, sq), (wk, sk), (wv, sv), (wo, so)])]
    for load in loads:
        load.start()

    barrier = pltpu.get_barrier_semaphore()

    def greet(k, carry):
        pl.semaphore_signal(barrier, inc=1, device_id=((f + k) % F, r), device_id_type=MESH)
        return carry

    lax.fori_loop(1, F, greet, 0)
    for rr in (up, down):
        for ff in (west, f, east):
            pl.semaphore_signal(barrier, inc=1, device_id=(ff, rr), device_id_type=MESH)

    fwd[...] = one_hot(lambda a: (a % T) * 16 + a // T)
    bwd[...] = one_hot(lambda a: (a % 16) * T + a // 16)
    pl.semaphore_wait(barrier, F - 1 + 6)
    loads[0].wait()

    def in_copy(k):
        peer = (f + k) % F
        return pltpu.make_async_remote_copy(
            vloc.at[:, :, snake(peer)], rin.at[f], in_send.at[k], in_recv.at[f],
            device_id=(peer, r), device_id_type=MESH)

    def in_start(k, carry):
        in_copy(k).start()
        return carry

    lax.fori_loop(1, F, in_start, 0)
    rin[f] = vloc[:, :, g]

    def in_wait(k, carry):
        src = (f + k) % F
        pltpu.make_async_remote_copy(
            vloc.at[:, :, snake(src)], rin.at[src], in_send.at[k], in_recv.at[src],
            device_id=(src, r), device_id_type=MESH).wait()
        return carry

    lax.fori_loop(1, F, in_wait, 0)

    loads[1].wait()
    x = dot(fwd[...], rin[...].reshape(512, C))
    xres[...] = x.astype(BF).reshape(2, PATCH, T, C)
    act_a[1:3, 1 : PATCH + 1] = silu(rms(x, ga[...])).astype(BF).reshape(2, PATCH, T, C)

    def halo(buf, send, recv):
        mid = pl.ds(1, PATCH)
        plan = [
            (buf.at[1, mid], buf.at[3, mid], (f, up)),
            (buf.at[2, mid], buf.at[0, mid], (f, down)),
            (buf.at[pl.ds(1, 2), 1], buf.at[pl.ds(1, 2), PATCH + 1], (west, r)),
            (buf.at[pl.ds(1, 2), PATCH], buf.at[pl.ds(1, 2), 0], (east, r)),
            (buf.at[1, 1], buf.at[3, PATCH + 1], (west, up)),
            (buf.at[1, PATCH], buf.at[3, 0], (east, up)),
            (buf.at[2, 1], buf.at[0, PATCH + 1], (west, down)),
            (buf.at[2, PATCH], buf.at[0, 0], (east, down)),
        ]
        copies = [
            pltpu.make_async_remote_copy(
                src, dst, send.at[n], recv.at[n], device_id=to, device_id_type=MESH)
            for n, (src, dst, to) in enumerate(plan)
        ]
        for copy in copies:
            copy.start()
        return copies

    def halo_end(buf, copies):
        for copy in copies:
            copy.wait()

        @pl.when(r == 0)
        def _():
            buf[0] = jnp.zeros((PATCH + 2, T, C), BF)

        @pl.when(r == R - 1)
        def _():
            buf[3] = jnp.zeros((PATCH + 2, T, C), BF)

        @pl.when(g == 0)
        def _():
            buf[:, 0] = jnp.zeros((4, T, C), BF)

        @pl.when(g == F - 1)
        def _():
            buf[:, PATCH + 1] = jnp.zeros((4, T, C), BF)

    copies = halo(act_a, ha_send, ha_recv)
    for load in loads[2:]:
        load.wait()
    halo_end(act_a, copies)

    def conv_one(row, carry):
        inner = conv_rows(act_a, ka, row).astype(BF).astype(F32)
        act = silu(rms(inner, gb[...])).astype(BF)
        act_b[row + 1, 1 : PATCH + 1] = act.reshape(PATCH, T, C)
        return carry

    lax.fori_loop(0, 2, conv_one, 0)
    copies = halo(act_b, hb_send, hb_recv)
    halo_end(act_b, copies)

    def conv_two(row, carry):
        res = xres[row].reshape(PATCH * T, C).astype(F32)
        block = (res + conv_rows(act_b, kb, row)).astype(BF)
        blk[row] = block.reshape(PATCH, T, C)
        normed = rms(block.astype(F32), gc[...]).astype(BF)
        for w, dst in ((sq, qs), (sk, ks), (sv, vs)):
            dst[pl.ds(row * PATCH, PATCH)] = dot(normed, w[...]).astype(BF).reshape(PATCH, T, C)
        return carry

    lax.fori_loop(0, 2, conv_two, 0)

    def attend(p, carry):
        for n in range(2):
            at = 2 * p + n
            low, high = attend_pixel(qs[at], ks[at], vs[at])
            att[at, :, 0:128] = low
            att[at, :, 128:256] = high
        return carry

    lax.fori_loop(0, 8, attend, 0)

    projected = dot(att[...].reshape(512, C), so[...]).astype(BF).astype(F32)
    encoded = (blk[...].reshape(512, C).astype(F32) + projected).astype(BF)
    sbuf[...] = dot(bwd[...], encoded).astype(BF).reshape(F, 2, 2, PATCH, C)

    def out_start(k, carry):
        peer = (f + k) % F
        pltpu.make_async_remote_copy(
            sbuf.at[peer], out.at[:, :, g], out_send.at[k], out_recv.at[f],
            device_id=(peer, r), device_id_type=MESH).start()
        return carry

    lax.fori_loop(1, F, out_start, 0)
    own = pltpu.make_async_copy(sbuf.at[f], out.at[:, :, g], lsem.at[0])
    own.start()

    def out_wait(k, carry):
        src = (f + k) % F
        pltpu.make_async_remote_copy(
            sbuf.at[src], out.at[:, :, snake(src)], out_send.at[k], out_recv.at[src],
            device_id=(src, r), device_id_type=MESH).wait()
        return carry

    lax.fori_loop(1, F, out_wait, 0)
    own.wait()


def shards(video, na, ca, nb, cb, nc, wq, wk, wv, wo):
    any_spec = pl.BlockSpec(memory_space=pl.ANY)
    dma = pltpu.SemaphoreType.DMA
    vm = pltpu.VMEM
    pix = (2 * PATCH, T, C)
    halo = (4, PATCH + 2, T, C)
    out = pl.pallas_call(
        kernel,
        out_shape=jax.ShapeDtypeStruct((2, 2, F, PATCH, C), BF),
        in_specs=[any_spec] * 10,
        out_specs=any_spec,
        scratch_shapes=[
            vm((2, 2, F, PATCH, C), BF), vm((F, 2, 2, PATCH, C), BF), vm((2, PATCH, T, C), BF),
            vm(halo, BF), vm(halo, BF), vm((27, C, C), BF), vm((27, C, C), BF),
            vm((1, C), F32), vm((1, C), F32), vm((1, C), F32),
            vm((C, C), BF), vm((C, C), BF), vm((C, C), BF), vm((C, C), BF),
            vm((512, 512), BF), vm((512, 512), BF),
            vm(pix, BF), vm(pix, BF), vm(pix, BF), vm(pix, BF), vm((2, PATCH, T, C), BF),
            vm((F, 2, 2, PATCH, C), BF),
            dma((10,)), dma((F,)), dma((F,)), dma((8,)), dma((8,)), dma((8,)), dma((8,)),
            dma((F,)), dma((F,)),
        ],
        compiler_params=pltpu.CompilerParams(
            collective_id=0, has_side_effects=True, vmem_limit_bytes=60 * 1024 * 1024),
    )(
        video.reshape(2, 2, F, PATCH, C), na.reshape(1, C), ca.reshape(27, C, C), nb.reshape(1, C),
        cb.reshape(27, C, C), nc.reshape(1, C), wq, wk, wv, wo,
    )
    return out.reshape(2, 2, F * PATCH, C)


def solution(mesh):
    placed = (P("frames", "rows", None, None), P(), P(), P(), P(), P(), P(), P(), P(), P())
    return jax.shard_map(
        shards,
        mesh=mesh,
        in_specs=placed,
        out_specs=P("frames", "rows", None, None),
        check_vma=False,
    )
```

```python
import functools

import jax
import jax.numpy as jnp
from jax import lax
from jax.experimental import pallas as pl
from jax.experimental.pallas import tpu as pltpu
from jax.sharding import PartitionSpec as P

MESH = pl.DeviceIdType.MESH
HEADS = 8
C = 256
T = 32
H = 16
F = 16
R = 16
PATCH = 8
BF = jnp.bfloat16
F32 = jnp.float32


def snake(i):
    half = i // 8
    return i + half * (23 - 2 * i)


def rms(x, gain):
    ms = jnp.mean(x * x, axis=-1, keepdims=True)
    return x * lax.rsqrt(ms + 1e-06) * gain


def silu(x):
    h = 0.5 * x
    return h + h * jnp.tanh(h)


def dot(a, b):
    return jnp.dot(a, b, preferred_element_type=F32)


def dot_tt(a, b, dims):
    return lax.dot_general(a, b, (dims, ((), ())), preferred_element_type=F32)


def conv_half(act, kern, y1, y0, h):
    slabs = [
        act[h, j : j + 2, l : l + PATCH].reshape(256, C) for j in range(3) for l in range(3)
    ]
    parts = []
    for i in range(3):
        total = dot(slabs[0], kern[i * 9])
        for n in range(1, 9):
            total = total + dot(slabs[n], kern[i * 9 + n])
        parts.append(total)
    at = 8 + H * h
    y1[:, at : at + H] = parts[1].reshape(16, H, C)
    y0[:, at : at + H] = parts[0].reshape(16, H, C)
    late = y1[:, at - 1 : at - 1 + H] + y0[:, at - 2 : at - 2 + H]
    return parts[2] + late.reshape(256, C)


def iota(shape, dim):
    return lax.broadcasted_iota(jnp.int32, shape, dim)


def attend_half(h, qs, ks, vs, att, hmask):
    keys = H * (h + 1)
    group = 128 // keys
    scale = 32 ** -0.5
    causal = iota((1, keys, 128), 1) <= (iota((1, keys, 128), 2) & 15) + H * h
    lane_head = iota((H, 128), 1) >> 5
    row_pixel = iota((128, 128), 0) >> (4 + h)
    for u in range(16 // group):
        pixels = range(u * group, (u + 1) * group)
        scores = []
        for p in pixels:
            q_bd = jnp.concatenate([qs[h, p]] * 8, axis=0) * hmask[...]
            scores.append(dot_tt(ks[p, 0:keys], q_bd, ((1,), (1,))))
        s = jnp.concatenate(scores, axis=0).reshape(group, keys, 128)
        s = jnp.where(causal, s, -1e30)
        e = jnp.exp((s - jnp.max(s, axis=1, keepdims=True)) * scale)
        probs = (e * (1.0 / jnp.sum(e, axis=1, keepdims=True))).astype(BF)
        probs = probs.reshape(128, 128).T
        value = vs[pl.ds(u * group, group), 0:keys].reshape(128, C)
        for hh in range(2):
            lanes = slice(128 * hh, 128 * hh + 128)
            part = value[:, lanes]
            v_bd = jnp.concatenate(
                [part * (row_pixel == n).astype(BF) for n in range(group)], axis=1)
            o = dot(probs[64 * hh : 64 * hh + 64], v_bd)
            for n, p in enumerate(pixels):
                tile = o[:, 128 * n : 128 * n + 128]
                got = tile[0:16]
                for k in range(1, 4):
                    got = jnp.where(lane_head == k, tile[16 * k : 16 * k + 16], got)
                att[p, :, lanes] = got.astype(BF)


def kernel(video, na, ca, nb, cb, nc, wq, wk, wv, wo, out,
           vloc, rin, xres, act_a, act_b, ka, kb, ga, gb, gc, sq, sk, sv, so,
           perm, hmask, y1, y0, qs, ks, vs, att, blk, sbuf,
           lsem, in_send, in_recv, ha_send, ha_recv, hb_send, hb_recv, out_send, out_recv):
    f = lax.axis_index("frames")
    r = lax.axis_index("rows")
    g = snake(f)
    mine = f // 8
    up, down = (r + R - 1) % R, (r + 1) % R
    west, east = snake((g + F - 1) % F), snake((g + 1) % F)

    loads = [pltpu.make_async_copy(src, dst, lsem.at[n]) for n, (src, dst) in enumerate(
        [(video, vloc), (na, ga), (ca, ka), (nb, gb), (cb, kb), (nc, gc),
         (wq, sq), (wk, sk), (wv, sv), (wo, so)])]
    for load in loads:
        load.start()

    barrier = pltpu.get_barrier_semaphore()

    def greet(k, carry):
        pl.semaphore_signal(barrier, inc=1, device_id=((f + k) % F, r), device_id_type=MESH)
        return carry

    lax.fori_loop(1, F, greet, 0)
    for rr in (up, down):
        for ff in (west, f, east):
            pl.semaphore_signal(barrier, inc=1, device_id=(ff, rr), device_id_type=MESH)

    a, b = iota((256, 256), 0), iota((256, 256), 1)
    perm[...] = jnp.where(b == ((a & 15) << 4) + (a >> 4), 1.0, 0.0).astype(BF)
    hmask[...] = jnp.where(
        (iota((128, C), 0) >> 4) == (iota((128, C), 1) >> 5), 1.0, 0.0).astype(BF)
    y1[:, 0:8] = jnp.zeros((16, 8, C), F32)
    y0[:, 0:8] = jnp.zeros((16, 8, C), F32)
    pl.semaphore_wait(barrier, F - 1 + 6)
    loads[0].wait()

    def in_copy(k, peer, source):
        return pltpu.make_async_remote_copy(
            vloc.at[:, :, snake(peer)], rin.at[source], in_send.at[k], in_recv.at[source],
            device_id=(peer, r), device_id_type=MESH)

    def in_start(k, carry):
        in_copy(k, (f + k) % F, f).start()
        return carry

    lax.fori_loop(1, F, in_start, 0)
    rin[f] = vloc[:, :, g]
    for load in loads[1:]:
        load.wait()


    def halo(buf, send, recv, h):
        b = buf.at[h]
        mid = pl.ds(1, PATCH)
        plan = [
            (b.at[1, mid], b.at[3, mid], (f, up)),
            (b.at[2, mid], b.at[0, mid], (f, down)),
            (b.at[pl.ds(1, 2), 1], b.at[pl.ds(1, 2), PATCH + 1], (west, r)),
            (b.at[pl.ds(1, 2), PATCH], b.at[pl.ds(1, 2), 0], (east, r)),
            (b.at[1, 1], b.at[3, PATCH + 1], (west, up)),
            (b.at[1, PATCH], b.at[3, 0], (east, up)),
            (b.at[2, 1], b.at[0, PATCH + 1], (west, down)),
            (b.at[2, PATCH], b.at[0, 0], (east, down)),
        ]
        copies = [
            pltpu.make_async_remote_copy(
                src, dst, send.at[8 * h + n], recv.at[8 * h + n],
                device_id=to, device_id_type=MESH)
            for n, (src, dst, to) in enumerate(plan)
        ]
        for copy in copies:
            copy.start()
        return copies

    def halo_end(buf, copies, h):
        for copy in copies:
            copy.wait()

        @pl.when(r == 0)
        def _():
            buf[h, 0] = jnp.zeros((PATCH + 2, H, C), BF)

        @pl.when(r == R - 1)
        def _():
            buf[h, 3] = jnp.zeros((PATCH + 2, H, C), BF)

        @pl.when(g == 0)
        def _():
            buf[h, :, 0] = jnp.zeros((4, H, C), BF)

        @pl.when(g == F - 1)
        def _():
            buf[h, :, PATCH + 1] = jnp.zeros((4, H, C), BF)

    halos_a, halos_b = [], []
    for h in range(2):
        def in_wait(k, carry):
            src = 8 * h + k

            @pl.when(src != f)
            def _():
                in_copy(0, src, src).wait_recv()
            return carry

        lax.fori_loop(0, 8, in_wait, 0)
        x = dot(perm[...], rin[8 * h : 8 * h + 8].reshape(256, C))
        xres[h] = x.astype(BF)
        act = silu(rms(x, ga[...])).astype(BF)
        act_a[h, 1:3, 1 : PATCH + 1] = act.reshape(2, PATCH, H, C)
        halos_a.append(halo(act_a, ha_send, ha_recv, h))

    for h in range(2):
        halo_end(act_a, halos_a[h], h)
        inner = conv_half(act_a, ka, y1, y0, h).astype(BF).astype(F32)
        act = silu(rms(inner, gb[...])).astype(BF)
        act_b[h, 1:3, 1 : PATCH + 1] = act.reshape(2, PATCH, H, C)
        halos_b.append(halo(act_b, hb_send, hb_recv, h))

    def out_copy(dst, source, k):
        return pltpu.make_async_remote_copy(
            sbuf.at[dst], out.at[:, :, snake(source)], out_send.at[k], out_recv.at[source],
            device_id=(dst, r), device_id_type=MESH)

    own = pltpu.make_async_copy(sbuf.at[f], out.at[:, :, g], lsem.at[0])
    for h in range(2):
        halo_end(act_b, halos_b[h], h)
        block = (xres[h].astype(F32) + conv_half(act_b, kb, y1, y0, h)).astype(BF)
        blk[...] = block
        normed = rms(block.astype(F32), gc[...]).astype(BF)
        qs[h] = dot(normed, sq[...]).astype(BF).reshape(16, H, C)
        ks[:, H * h : H * h + H] = dot(normed, sk[...]).astype(BF).reshape(16, H, C)
        vs[:, H * h : H * h + H] = dot(normed, sv[...]).astype(BF).reshape(16, H, C)
        attend_half(h, qs, ks, vs, att, hmask)
        projected = dot(att[...].reshape(256, C), so[...]).astype(BF).astype(F32)
        encoded = (blk[...].astype(F32) + projected).astype(BF)
        sbuf[8 * h : 8 * h + 8] = dot(perm[...], encoded).astype(BF).reshape(8, 2, 2, PATCH, C)

        @pl.when(mine == h)
        def _():
            own.start()

        @pl.when(mine != h)
        def _():
            out_copy(8 * h + f % 8, f, 8 * h).start()

        def out_start(k, carry):
            out_copy(8 * h + (f + k) % 8, f, 8 * h + k).start()
            return carry

        lax.fori_loop(1, 8, out_start, 0)

    def finish(k, carry):
        src = (f + k) % F
        in_copy(k, src, src).wait_send()
        out_copy(src, src, k).wait_recv()
        return carry

    lax.fori_loop(1, F, finish, 0)
    own.wait()

    def sent(k, carry):
        @pl.when(k != 8 * mine)
        def _():
            out_copy((f + 1) % F, f, k).wait_send()
        return carry

    lax.fori_loop(0, F, sent, 0)


def shards(video, na, ca, nb, cb, nc, wq, wk, wv, wo):
    any_spec = pl.BlockSpec(memory_space=pl.ANY)
    dma = pltpu.SemaphoreType.DMA
    vm = pltpu.VMEM
    halo = (2, 4, PATCH + 2, H, C)
    out = pl.pallas_call(
        kernel,
        out_shape=jax.ShapeDtypeStruct((2, 2, F, PATCH, C), BF),
        in_specs=[any_spec] * 10,
        out_specs=any_spec,
        scratch_shapes=[
            vm((2, 2, F, PATCH, C), BF), vm((F, 2, 2, PATCH, C), BF), vm((2, 256, C), BF),
            vm(halo, BF), vm(halo, BF), vm((27, C, C), BF), vm((27, C, C), BF),
            vm((1, C), F32), vm((1, C), F32), vm((1, C), F32),
            vm((C, C), BF), vm((C, C), BF), vm((C, C), BF), vm((C, C), BF),
            vm((256, 256), BF), vm((128, C), BF), vm((16, 40, C), F32), vm((16, 40, C), F32),
            vm((2, 16, H, C), BF), vm((16, T, C), BF), vm((16, T, C), BF), vm((16, H, C), BF),
            vm((256, C), BF), vm((F, 2, 2, PATCH, C), BF),
            dma((10,)), dma((F,)), dma((F,)), dma((16,)), dma((16,)), dma((16,)), dma((16,)),
            dma((F,)), dma((F,)),
        ],
        compiler_params=pltpu.CompilerParams(
            collective_id=0, has_side_effects=True, vmem_limit_bytes=60 * 1024 * 1024),
    )(
        video.reshape(2, 2, F, PATCH, C), na.reshape(1, C), ca.reshape(27, C, C), nb.reshape(1, C),
        cb.reshape(27, C, C), nc.reshape(1, C), wq, wk, wv, wo,
    )
    return out.reshape(2, 2, F * PATCH, C)


def solution(mesh):
    placed = (P("frames", "rows", None, None), P(), P(), P(), P(), P(), P(), P(), P(), P())
    return jax.shard_map(
        shards,
        mesh=mesh,
        in_specs=placed,
        out_specs=P("frames", "rows", None, None),
        check_vma=False,
    )
```

```python
import functools

import jax
import jax.numpy as jnp
from jax import lax
from jax.experimental import pallas as pl
from jax.experimental.pallas import tpu as pltpu
from jax.sharding import PartitionSpec as P

MESH = pl.DeviceIdType.MESH
HEADS = 8
C = 256
T = 32
H = 16
F = 16
R = 16
PATCH = 8
BF = jnp.bfloat16
F32 = jnp.float32


def snake(i):
    half = i // 8
    return i + half * (23 - 2 * i)


def rms(x, gain):
    ms = jnp.mean(x * x, axis=-1, keepdims=True)
    return x * lax.rsqrt(ms + 1e-06) * gain


def silu(x):
    h = 0.5 * x
    return h + h * jnp.tanh(h)


def dot(a, b):
    return jnp.dot(a, b, preferred_element_type=F32)


def dot_tt(a, b, dims):
    return lax.dot_general(a, b, (dims, ((), ())), preferred_element_type=F32)


def inner_taps(act, kern, ys, h):
    slabs = [
        act[h, j : j + 2, l : l + PATCH].reshape(256, C) for j in range(3) for l in range(3)
    ]
    at = 8 + H * h
    for i in range(3):
        total = dot(slabs[0], kern[i * 9])
        for n in range(1, 9):
            total = total + dot(slabs[n], kern[i * 9 + n])
        ys[i, :, at : at + H] = total.reshape(16, H, C)


def edge_taps(north, south, west, east, kern, ys, h):
    rows = slice(8 + H * h, 8 + H * h + H)

    def chain(terms):
        total = None
        for lhs, tap in terms:
            term = dot(lhs.reshape(-1, C), kern[tap])
            total = term if total is None else total + term
        return total

    for i in range(3):
        top = chain([(north[h, l : l + PATCH], i * 9 + l) for l in range(3)])
        low = chain([(south[h, l : l + PATCH], i * 9 + 6 + l) for l in range(3)])
        left = chain([(west[h, j : j + 2], i * 9 + 3 * j) for j in range(3)])
        right = chain([(east[h, j : j + 2], i * 9 + 3 * j + 2) for j in range(3)])
        ys[i, 0:8, rows] += top.reshape(8, H, C)
        ys[i, 8:16, rows] += low.reshape(8, H, C)
        for row in range(2):
            ys[i, 8 * row, rows] += left[H * row : H * row + H]
            ys[i, 8 * row + 7, rows] += right[H * row : H * row + H]
    at = 8 + H * h
    total = ys[2, :, at : at + H] + ys[1, :, at - 1 : at - 1 + H] + ys[0, :, at - 2 : at - 2 + H]
    return total.reshape(256, C)


def iota(shape, dim):
    return lax.broadcasted_iota(jnp.int32, shape, dim)


def attend_row(h, row, qs, ks, vs, att, hmask):
    keys = H * (h + 1)
    group = 128 // keys
    scale = 32 ** -0.5
    causal = iota((1, keys, 128), 1) <= (iota((1, keys, 128), 2) & 15) + H * h
    lane_head = iota((H, 128), 1) >> 5
    row_pixel = iota((128, 128), 0) >> (4 + h)
    for u in range(row * 8 // group, (row + 1) * 8 // group):
        pixels = range(u * group, (u + 1) * group)
        scores = []
        for p in pixels:
            q_bd = jnp.concatenate([qs[h, p]] * 8, axis=0) * hmask[...]
            scores.append(dot_tt(ks[p, 0:keys], q_bd, ((1,), (1,))))
        s = jnp.concatenate(scores, axis=0).reshape(group, keys, 128)
        s = jnp.where(causal, s, -1e30)
        e = jnp.exp((s - jnp.max(s, axis=1, keepdims=True)) * scale)
        probs = (e * (1.0 / jnp.sum(e, axis=1, keepdims=True))).astype(BF)
        probs = probs.reshape(128, 128).T
        value = vs[pl.ds(u * group, group), 0:keys].reshape(128, C)
        for hh in range(2):
            lanes = slice(128 * hh, 128 * hh + 128)
            part = value[:, lanes]
            v_bd = jnp.concatenate(
                [part * (row_pixel == n).astype(BF) for n in range(group)], axis=1)
            o = dot(probs[64 * hh : 64 * hh + 64], v_bd)
            for n, p in enumerate(pixels):
                tile = o[:, 128 * n : 128 * n + 128]
                got = tile[0:16]
                for k in range(1, 4):
                    got = jnp.where(lane_head == k, tile[16 * k : 16 * k + 16], got)
                att[p, :, lanes] = got.astype(BF)


def kernel(video, na, ca, nb, cb, nc, wq, wk, wv, wo, out,
           vloc, rin, xres, act_a, act_b, ka, kb, ga, gb, gc, sq, sk, sv, so,
           perm, perm_row, hmask, ya, yb, na_h, sa_h, wa_h, ea_h, nb_h, sb_h, wb_h, eb_h, qs, ks, vs, att, blk, sbuf,
           lsem, in_send, in_recv, ha_send, ha_recv, hb_send, hb_recv, out_send, out_recv):
    f = lax.axis_index("frames")
    r = lax.axis_index("rows")
    g = snake(f)
    mine = f // 8
    up, down = (r + R - 1) % R, (r + 1) % R
    west, east = snake((g + F - 1) % F), snake((g + 1) % F)

    loads = [pltpu.make_async_copy(src, dst, lsem.at[n]) for n, (src, dst) in enumerate(
        [(video, vloc), (na, ga), (ca, ka), (nb, gb), (cb, kb), (nc, gc),
         (wq, sq), (wk, sk), (wv, sv), (wo, so)])]
    for load in loads:
        load.start()

    barrier = pltpu.get_barrier_semaphore()

    def greet(k, carry):
        pl.semaphore_signal(barrier, inc=1, device_id=((f + k) % F, r), device_id_type=MESH)
        return carry

    lax.fori_loop(1, F, greet, 0)
    for rr in (up, down):
        for ff in (west, f, east):
            pl.semaphore_signal(barrier, inc=1, device_id=(ff, rr), device_id_type=MESH)

    a, b = iota((256, 256), 0), iota((256, 256), 1)
    perm[...] = jnp.where(b == ((a & 15) << 4) + (a >> 4), 1.0, 0.0).astype(BF)
    hmask[...] = jnp.where(
        (iota((128, C), 0) >> 4) == (iota((128, C), 1) >> 5), 1.0, 0.0).astype(BF)
    a, b = iota((128, 128), 0), iota((128, 128), 1)
    perm_row[...] = jnp.where(b == ((a & 7) << 4) + (a >> 3), 1.0, 0.0).astype(BF)
    for ys in (ya, yb):
        ys[:, :, 0:8] = jnp.zeros((3, 16, 8, C), F32)
    for buf in (act_a, act_b):
        for at in (0, 3):
            buf[:, at] = jnp.zeros((2, PATCH + 2, H, C), BF)
        for at in (0, PATCH + 1):
            buf[:, 1:3, at] = jnp.zeros((2, 2, H, C), BF)
    for buf in (wa_h, ea_h, wb_h, eb_h):
        for at in (0, 3):
            buf[:, at] = jnp.zeros((2, H, C), BF)
    pl.semaphore_wait(barrier, F - 1 + 6)
    loads[0].wait()

    def in_copy(k, peer, source):
        return pltpu.make_async_remote_copy(
            vloc.at[:, :, snake(peer)], rin.at[source], in_send.at[k], in_recv.at[source],
            device_id=(peer, r), device_id_type=MESH)

    def in_start(k, carry):
        in_copy(k, (f + k) % F, f).start()
        return carry

    lax.fori_loop(1, F, in_start, 0)
    rin[f] = vloc[:, :, g]
    for load in loads[1:]:
        load.wait()


    def halo(buf, lands, send, recv, h):
        b = buf.at[h]
        north, south, west_h, east_h = (land.at[h] for land in lands)
        mid, two = pl.ds(1, PATCH), pl.ds(1, 2)
        plan = [
            (b.at[1, mid], south.at[mid], (f, up)),
            (b.at[2, mid], north.at[mid], (f, down)),
            (b.at[1, 1], south.at[PATCH + 1], (west, up)),
            (b.at[1, PATCH], south.at[0], (east, up)),
            (b.at[2, 1], north.at[PATCH + 1], (west, down)),
            (b.at[2, PATCH], north.at[0], (east, down)),
            (b.at[two, 1], east_h.at[two], (west, r)),
            (b.at[two, PATCH], west_h.at[two], (east, r)),
        ]
        copies = [
            pltpu.make_async_remote_copy(
                src, dst, send.at[8 * h + n], recv.at[8 * h + n],
                device_id=to, device_id_type=MESH)
            for n, (src, dst, to) in enumerate(plan)
        ]
        for copy in copies:
            copy.start()
        return copies

    def halo_end(lands, copies, h):
        for copy in copies:
            copy.wait()
        north, south, west_h, east_h = lands

        @pl.when(r == 0)
        def _():
            north[h] = jnp.zeros((PATCH + 2, H, C), BF)

        @pl.when(r == R - 1)
        def _():
            south[h] = jnp.zeros((PATCH + 2, H, C), BF)

        @pl.when(g == 0)
        def _():
            north[h, 0] = jnp.zeros((H, C), BF)
            south[h, 0] = jnp.zeros((H, C), BF)
            west_h[h, 1:3] = jnp.zeros((2, H, C), BF)

        @pl.when(g == F - 1)
        def _():
            north[h, PATCH + 1] = jnp.zeros((H, C), BF)
            south[h, PATCH + 1] = jnp.zeros((H, C), BF)
            east_h[h, 1:3] = jnp.zeros((2, H, C), BF)

    lands_a = (na_h, sa_h, wa_h, ea_h)
    lands_b = (nb_h, sb_h, wb_h, eb_h)
    halos_a, halos_b = [], []
    for h in range(2):
        def in_wait(k, carry):
            src = 8 * h + k

            @pl.when(src != f)
            def _():
                in_copy(0, src, src).wait_recv()
            return carry

        lax.fori_loop(0, 8, in_wait, 0)
        x = dot(perm[...], rin[8 * h : 8 * h + 8].reshape(256, C))
        xres[h] = x.astype(BF)
        act = silu(rms(x, ga[...])).astype(BF)
        act_a[h, 1:3, 1 : PATCH + 1] = act.reshape(2, PATCH, H, C)
        halos_a.append(halo(act_a, lands_a, ha_send, ha_recv, h))

    for h in range(2):
        inner_taps(act_a, ka, ya, h)
    for h in range(2):
        halo_end(lands_a, halos_a[h], h)
        inner = edge_taps(*lands_a, ka, ya, h).astype(BF).astype(F32)
        act = silu(rms(inner, gb[...])).astype(BF)
        act_b[h, 1:3, 1 : PATCH + 1] = act.reshape(2, PATCH, H, C)
        halos_b.append(halo(act_b, lands_b, hb_send, hb_recv, h))
    for h in range(2):
        inner_taps(act_b, kb, yb, h)

    def out_copy(dst, source, row, k):
        return pltpu.make_async_remote_copy(
            sbuf.at[dst, row], out.at[:, row, snake(source)],
            out_send.at[2 * k + row], out_recv.at[2 * source + row],
            device_id=(dst, r), device_id_type=MESH)

    own = [pltpu.make_async_copy(sbuf.at[f, row], out.at[:, row, g], lsem.at[row])
           for row in range(2)]
    for h in range(2):
        halo_end(lands_b, halos_b[h], h)
        block = (xres[h].astype(F32) + edge_taps(*lands_b, kb, yb, h)).astype(BF)
        blk[...] = block
        normed = rms(block.astype(F32), gc[...]).astype(BF)
        qs[h] = dot(normed, sq[...]).astype(BF).reshape(16, H, C)
        ks[:, H * h : H * h + H] = dot(normed, sk[...]).astype(BF).reshape(16, H, C)
        vs[:, H * h : H * h + H] = dot(normed, sv[...]).astype(BF).reshape(16, H, C)
        for row in range(2):
            attend_row(h, row, qs, ks, vs, att, hmask)
            at = slice(128 * row, 128 * row + 128)
            projected = dot(att[8 * row : 8 * row + 8].reshape(128, C), so[...])
            encoded = (blk[at].astype(F32) + projected.astype(BF).astype(F32)).astype(BF)
            moved = dot(perm_row[...], encoded).astype(BF)
            sbuf[8 * h : 8 * h + 8, row] = moved.reshape(8, 2, PATCH, C)

            @pl.when(mine == h)
            def _():
                own[row].start()

            def out_start(k, carry):
                dst = 8 * h + k

                @pl.when(dst != f)
                def _():
                    out_copy(dst, f, row, dst).start()
                return carry

            lax.fori_loop(0, 8, out_start, 0)

    def finish(k, carry):
        src = (f + k) % F
        in_copy(k, src, src).wait_send()
        for row in range(2):
            out_copy(src, src, row, src).wait()
        return carry

    lax.fori_loop(1, F, finish, 0)
    for copy in own:
        copy.wait()


def shards(video, na, ca, nb, cb, nc, wq, wk, wv, wo):
    any_spec = pl.BlockSpec(memory_space=pl.ANY)
    dma = pltpu.SemaphoreType.DMA
    vm = pltpu.VMEM
    halo = (2, 4, PATCH + 2, H, C)
    lands = [vm((2, n, H, C), BF) for n in (PATCH + 2, PATCH + 2, 4, 4)]
    out = pl.pallas_call(
        kernel,
        out_shape=jax.ShapeDtypeStruct((2, 2, F, PATCH, C), BF),
        in_specs=[any_spec] * 10,
        out_specs=any_spec,
        scratch_shapes=[
            vm((2, 2, F, PATCH, C), BF), vm((F, 2, 2, PATCH, C), BF), vm((2, 256, C), BF),
            vm(halo, BF), vm(halo, BF), vm((27, C, C), BF), vm((27, C, C), BF),
            vm((1, C), F32), vm((1, C), F32), vm((1, C), F32),
            vm((C, C), BF), vm((C, C), BF), vm((C, C), BF), vm((C, C), BF),
            vm((256, 256), BF), vm((128, 128), BF), vm((128, C), BF),
            vm((3, 16, 40, C), F32), vm((3, 16, 40, C), F32),
            *lands, *lands,
            vm((2, 16, H, C), BF), vm((16, T, C), BF), vm((16, T, C), BF), vm((16, H, C), BF),
            vm((256, C), BF), vm((F, 2, 2, PATCH, C), BF),
            dma((10,)), dma((F,)), dma((F,)), dma((16,)), dma((16,)), dma((16,)), dma((16,)),
            dma((2 * F,)), dma((2 * F,)),
        ],
        compiler_params=pltpu.CompilerParams(
            collective_id=0, has_side_effects=True, vmem_limit_bytes=60 * 1024 * 1024),
    )(
        video.reshape(2, 2, F, PATCH, C), na.reshape(1, C), ca.reshape(27, C, C), nb.reshape(1, C),
        cb.reshape(27, C, C), nc.reshape(1, C), wq, wk, wv, wo,
    )
    return out.reshape(2, 2, F * PATCH, C)


def solution(mesh):
    placed = (P("frames", "rows", None, None), P(), P(), P(), P(), P(), P(), P(), P(), P())
    return jax.shard_map(
        shards,
        mesh=mesh,
        in_specs=placed,
        out_specs=P("frames", "rows", None, None),
        check_vma=False,
    )
```

```python
import functools

import jax
import jax.numpy as jnp
from jax import lax
from jax.experimental import pallas as pl
from jax.experimental.pallas import tpu as pltpu
from jax.sharding import PartitionSpec as P

MESH = pl.DeviceIdType.MESH
HEADS = 8
C = 256
T = 32
H = 16
F = 16
R = 16
PATCH = 8
BF = jnp.bfloat16
F32 = jnp.float32


def snake(i):
    half = i // 8
    return i + half * (23 - 2 * i)


def band_of(r):
    odd, x_low = (r // 4) % 2, (r // 2) % 2
    return r + odd * (2 - 4 * x_low)


def rms(x, gain):
    ms = jnp.mean(x * x, axis=-1, keepdims=True)
    return x * lax.rsqrt(ms + 1e-06) * gain


def silu(x):
    h = 0.5 * x
    return h + h * jnp.tanh(h)


def dot(a, b):
    return jnp.dot(a, b, preferred_element_type=F32)


def dot_tt(a, b, dims):
    return lax.dot_general(a, b, (dims, ((), ())), preferred_element_type=F32)


def inner_taps(act, kern, ys, h):
    slabs = [
        act[h, j : j + 2, l : l + PATCH].reshape(256, C) for j in range(3) for l in range(3)
    ]
    at = 8 + H * h
    for i in range(3):
        total = dot(slabs[0], kern[i * 9])
        for n in range(1, 9):
            total = total + dot(slabs[n], kern[i * 9 + n])
        ys[i, :, at : at + H] = total.reshape(16, H, C)


def edge_taps(north, south, west, east, kern, ys, h):
    rows = slice(8 + H * h, 8 + H * h + H)

    def chain(terms):
        total = None
        for lhs, tap in terms:
            term = dot(lhs.reshape(-1, C), kern[tap])
            total = term if total is None else total + term
        return total

    for i in range(3):
        top = chain([(north[h, l : l + PATCH], i * 9 + l) for l in range(3)])
        low = chain([(south[h, l : l + PATCH], i * 9 + 6 + l) for l in range(3)])
        left = chain([(west[h, j : j + 2], i * 9 + 3 * j) for j in range(3)])
        right = chain([(east[h, j : j + 2], i * 9 + 3 * j + 2) for j in range(3)])
        ys[i, 0:8, rows] += top.reshape(8, H, C)
        ys[i, 8:16, rows] += low.reshape(8, H, C)
        for row in range(2):
            ys[i, 8 * row, rows] += left[H * row : H * row + H]
            ys[i, 8 * row + 7, rows] += right[H * row : H * row + H]
    at = 8 + H * h
    total = ys[2, :, at : at + H] + ys[1, :, at - 1 : at - 1 + H] + ys[0, :, at - 2 : at - 2 + H]
    return total.reshape(256, C)


def iota(shape, dim):
    return lax.broadcasted_iota(jnp.int32, shape, dim)


def attend_row(h, row, qs, ks, vs, att, hmask):
    keys = H * (h + 1)
    group = 128 // keys
    scale = 32 ** -0.5
    causal = iota((1, keys, 128), 1) <= (iota((1, keys, 128), 2) & 15) + H * h
    lane_head = iota((H, 128), 1) >> 5
    row_pixel = iota((128, 128), 0) >> (4 + h)
    for u in range(row * 8 // group, (row + 1) * 8 // group):
        pixels = range(u * group, (u + 1) * group)
        scores = []
        for p in pixels:
            q_bd = jnp.concatenate([qs[h, p]] * 8, axis=0) * hmask[...]
            scores.append(dot_tt(ks[p, 0:keys], q_bd, ((1,), (1,))))
        s = jnp.concatenate(scores, axis=0).reshape(group, keys, 128)
        s = jnp.where(causal, s, -1e30)
        e = jnp.exp((s - jnp.max(s, axis=1, keepdims=True)) * scale)
        probs = (e * (1.0 / jnp.sum(e, axis=1, keepdims=True))).astype(BF)
        probs = probs.reshape(128, 128).T
        value = vs[pl.ds(u * group, group), 0:keys].reshape(128, C)
        for hh in range(2):
            lanes = slice(128 * hh, 128 * hh + 128)
            part = value[:, lanes]
            v_bd = jnp.concatenate(
                [part * (row_pixel == n).astype(BF) for n in range(group)], axis=1)
            o = dot(probs[64 * hh : 64 * hh + 64], v_bd)
            for n, p in enumerate(pixels):
                tile = o[:, 128 * n : 128 * n + 128]
                got = tile[0:16]
                for k in range(1, 4):
                    got = jnp.where(lane_head == k, tile[16 * k : 16 * k + 16], got)
                att[p, :, lanes] = got.astype(BF)


def kernel(video, na, ca, nb, cb, nc, wq, wk, wv, wo, out,
           vloc, rin, xres, act_a, act_b, ka, kb, ga, gb, gc, sq, sk, sv, so,
           perm, perm_row, hmask, ya, yb, na_h, sa_h, wa_h, ea_h, nb_h, sb_h, wb_h, eb_h, qs, ks, vs, att, blk, sbuf,
           lsem, in_send, in_recv, ha_send, ha_recv, hb_send, hb_recv, out_send, out_recv):
    f = lax.axis_index("frames")
    r = lax.axis_index("rows")
    g = snake(f)
    mine = f // 8
    w = band_of(r)
    moved_band = (r // 4) % 2
    up, down = band_of((w + R - 1) % R), band_of((w + 1) % R)

    def remote(peer):
        return (peer != f) | (moved_band == 1)
    west, east = snake((g + F - 1) % F), snake((g + 1) % F)

    loads = [pltpu.make_async_copy(src, dst, lsem.at[n]) for n, (src, dst) in enumerate(
        [(video, vloc), (na, ga), (ca, ka), (nb, gb), (cb, kb), (nc, gc),
         (wq, sq), (wk, sk), (wv, sv), (wo, so)])]
    for load in loads:
        load.start()

    barrier = pltpu.get_barrier_semaphore()

    def greet(k, carry):
        @pl.when(remote(k))
        def _():
            pl.semaphore_signal(barrier, inc=1, device_id=(k, w), device_id_type=MESH)
        return carry

    lax.fori_loop(0, F, greet, 0)
    for ff in (west, east):
        pl.semaphore_signal(barrier, inc=1, device_id=(ff, r), device_id_type=MESH)
    for rr in (up, down):
        for ff in (west, f, east):
            pl.semaphore_signal(barrier, inc=1, device_id=(ff, rr), device_id_type=MESH)

    a, b = iota((256, 256), 0), iota((256, 256), 1)
    perm[...] = jnp.where(b == ((a & 15) << 4) + (a >> 4), 1.0, 0.0).astype(BF)
    hmask[...] = jnp.where(
        (iota((128, C), 0) >> 4) == (iota((128, C), 1) >> 5), 1.0, 0.0).astype(BF)
    a, b = iota((128, 128), 0), iota((128, 128), 1)
    perm_row[...] = jnp.where(b == ((a & 7) << 4) + (a >> 3), 1.0, 0.0).astype(BF)
    for ys in (ya, yb):
        ys[:, :, 0:8] = jnp.zeros((3, 16, 8, C), F32)
    for buf in (act_a, act_b):
        for at in (0, 3):
            buf[:, at] = jnp.zeros((2, PATCH + 2, H, C), BF)
        for at in (0, PATCH + 1):
            buf[:, 1:3, at] = jnp.zeros((2, 2, H, C), BF)
    for buf in (wa_h, ea_h, wb_h, eb_h):
        for at in (0, 3):
            buf[:, at] = jnp.zeros((2, H, C), BF)
    pl.semaphore_wait(barrier, F - 1 + moved_band + 8)
    loads[0].wait()

    def in_copy(k, peer, source):
        return pltpu.make_async_remote_copy(
            vloc.at[:, :, snake(peer)], rin.at[source], in_send.at[k], in_recv.at[source],
            device_id=(peer, w), device_id_type=MESH)

    def in_start(k, carry):
        peer = (f + k) % F

        @pl.when(remote(peer))
        def _():
            in_copy(k, peer, f).start()
        return carry

    lax.fori_loop(0, F, in_start, 0)

    @pl.when(moved_band == 0)
    def _():
        rin[f] = vloc[:, :, g]

    for load in loads[1:]:
        load.wait()


    def halo(buf, lands, send, recv, h):
        b = buf.at[h]
        north, south, west_h, east_h = (land.at[h] for land in lands)
        mid, two = pl.ds(1, PATCH), pl.ds(1, 2)
        plan = [
            (b.at[1, mid], south.at[mid], (f, up)),
            (b.at[2, mid], north.at[mid], (f, down)),
            (b.at[1, 1], south.at[PATCH + 1], (west, up)),
            (b.at[1, PATCH], south.at[0], (east, up)),
            (b.at[2, 1], north.at[PATCH + 1], (west, down)),
            (b.at[2, PATCH], north.at[0], (east, down)),
            (b.at[two, 1], east_h.at[two], (west, r)),
            (b.at[two, PATCH], west_h.at[two], (east, r)),
        ]
        copies = [
            pltpu.make_async_remote_copy(
                src, dst, send.at[8 * h + n], recv.at[8 * h + n],
                device_id=to, device_id_type=MESH)
            for n, (src, dst, to) in enumerate(plan)
        ]
        return copies

    def halo_start(copies, before=()):
        for copy in before:
            copy.wait_send()
        for copy in copies:
            copy.start()

    def halo_end(lands, copies, h):
        for copy in copies:
            copy.wait_recv()
        north, south, west_h, east_h = lands

        @pl.when(w == 0)
        def _():
            north[h] = jnp.zeros((PATCH + 2, H, C), BF)

        @pl.when(w == R - 1)
        def _():
            south[h] = jnp.zeros((PATCH + 2, H, C), BF)

        @pl.when(g == 0)
        def _():
            north[h, 0] = jnp.zeros((H, C), BF)
            south[h, 0] = jnp.zeros((H, C), BF)
            west_h[h, 1:3] = jnp.zeros((2, H, C), BF)

        @pl.when(g == F - 1)
        def _():
            north[h, PATCH + 1] = jnp.zeros((H, C), BF)
            south[h, PATCH + 1] = jnp.zeros((H, C), BF)
            east_h[h, 1:3] = jnp.zeros((2, H, C), BF)

    lands_a = (na_h, sa_h, wa_h, ea_h)
    lands_b = (nb_h, sb_h, wb_h, eb_h)
    halos_a, halos_b = [], []
    for h in range(2):
        def in_wait(k, carry):
            src = 8 * h + k

            @pl.when(remote(src))
            def _():
                in_copy(0, src, src).wait_recv()
            return carry

        lax.fori_loop(0, 8, in_wait, 0)
        x = dot(perm[...], rin[8 * h : 8 * h + 8].reshape(256, C))
        xres[h] = x.astype(BF)
        act = silu(rms(x, ga[...])).astype(BF)
        act_a[h, 1:3, 1 : PATCH + 1] = act.reshape(2, PATCH, H, C)
        halos_a.append(halo(act_a, lands_a, ha_send, ha_recv, h))
        if h == 0:
            halo_start(halos_a[0])

    inner_taps(act_a, ka, ya, 0)
    halo_start(halos_a[1], halos_a[0])
    inner_taps(act_a, ka, ya, 1)
    for h in range(2):
        halo_end(lands_a, halos_a[h], h)
        inner = edge_taps(*lands_a, ka, ya, h).astype(BF).astype(F32)
        act = silu(rms(inner, gb[...])).astype(BF)
        act_b[h, 1:3, 1 : PATCH + 1] = act.reshape(2, PATCH, H, C)
        halos_b.append(halo(act_b, lands_b, hb_send, hb_recv, h))
        halo_start(halos_b[h], halos_b[0] if h else halos_a[1])
    for h in range(2):
        inner_taps(act_b, kb, yb, h)

    def out_copy(dst, source, row, k):
        return pltpu.make_async_remote_copy(
            sbuf.at[dst, row], out.at[:, row, snake(source)],
            out_send.at[2 * k + row], out_recv.at[2 * source + row],
            device_id=(dst, w), device_id_type=MESH)

    own = [pltpu.make_async_copy(sbuf.at[f, row], out.at[:, row, g], lsem.at[row])
           for row in range(2)]
    for h in range(2):
        halo_end(lands_b, halos_b[h], h)
        block = (xres[h].astype(F32) + edge_taps(*lands_b, kb, yb, h)).astype(BF)
        blk[...] = block
        normed = rms(block.astype(F32), gc[...]).astype(BF)
        qs[h] = dot(normed, sq[...]).astype(BF).reshape(16, H, C)
        ks[:, H * h : H * h + H] = dot(normed, sk[...]).astype(BF).reshape(16, H, C)
        vs[:, H * h : H * h + H] = dot(normed, sv[...]).astype(BF).reshape(16, H, C)
        for row in range(2):
            attend_row(h, row, qs, ks, vs, att, hmask)
            at = slice(128 * row, 128 * row + 128)
            projected = dot(att[8 * row : 8 * row + 8].reshape(128, C), so[...])
            encoded = (blk[at].astype(F32) + projected.astype(BF).astype(F32)).astype(BF)
            moved = dot(perm_row[...], encoded).astype(BF)
            sbuf[8 * h : 8 * h + 8, row] = moved.reshape(8, 2, PATCH, C)

            @pl.when((mine == h) & (moved_band == 0))
            def _():
                own[row].start()

            def out_start(k, carry):
                dst = 8 * h + k

                @pl.when(remote(dst))
                def _():
                    out_copy(dst, f, row, dst).start()
                return carry

            lax.fori_loop(0, 8, out_start, 0)

    def finish(k, carry):
        src = (f + k) % F

        @pl.when(remote(src))
        def _():
            in_copy(k, src, src).wait_send()
            for row in range(2):
                out_copy(src, src, row, src).wait()
        return carry

    lax.fori_loop(0, F, finish, 0)
    for copy in halos_b[1]:
        copy.wait_send()

    @pl.when(moved_band == 0)
    def _():
        for copy in own:
            copy.wait()


def shards(video, na, ca, nb, cb, nc, wq, wk, wv, wo):
    any_spec = pl.BlockSpec(memory_space=pltpu.HBM)
    dma = pltpu.SemaphoreType.DMA
    vm = pltpu.VMEM
    halo = (2, 4, PATCH + 2, H, C)
    lands = [vm((2, n, H, C), BF) for n in (PATCH + 2, PATCH + 2, 4, 4)]
    out = pl.pallas_call(
        kernel,
        out_shape=pltpu.VMEM((2, 2, F, PATCH, C), BF),
        in_specs=[any_spec] * 10,
        out_specs=pl.BlockSpec(memory_space=pltpu.VMEM),
        scratch_shapes=[
            vm((2, 2, F, PATCH, C), BF), vm((F, 2, 2, PATCH, C), BF), vm((2, 256, C), BF),
            vm(halo, BF), vm(halo, BF), vm((27, C, C), BF), vm((27, C, C), BF),
            vm((1, C), F32), vm((1, C), F32), vm((1, C), F32),
            vm((C, C), BF), vm((C, C), BF), vm((C, C), BF), vm((C, C), BF),
            vm((256, 256), BF), vm((128, 128), BF), vm((128, C), BF),
            vm((3, 16, 40, C), F32), vm((3, 16, 40, C), F32),
            *lands, *lands,
            vm((2, 16, H, C), BF), vm((16, T, C), BF), vm((16, T, C), BF), vm((16, H, C), BF),
            vm((256, C), BF), vm((F, 2, 2, PATCH, C), BF),
            dma((10,)), dma((F,)), dma((F,)), dma((16,)), dma((16,)), dma((16,)), dma((16,)),
            dma((2 * F,)), dma((2 * F,)),
        ],
        compiler_params=pltpu.CompilerParams(
            collective_id=0, has_side_effects=True, vmem_limit_bytes=60 * 1024 * 1024),
    )(
        video.reshape(2, 2, F, PATCH, C), na.reshape(1, C), ca.reshape(27, C, C), nb.reshape(1, C),
        cb.reshape(27, C, C), nc.reshape(1, C), wq, wk, wv, wo,
    )
    return out.reshape(2, 2, F * PATCH, C)


def solution(mesh):
    placed = (P("frames", "rows", None, None), P(), P(), P(), P(), P(), P(), P(), P(), P())
    return jax.shard_map(
        shards,
        mesh=mesh,
        in_specs=placed,
        out_specs=P("frames", "rows", None, None),
        check_vma=False,
    )
```

```python
import functools

import jax
import jax.numpy as jnp
from jax import lax
from jax.experimental import pallas as pl
from jax.experimental.pallas import tpu as pltpu
from jax.sharding import PartitionSpec as P

MESH = pl.DeviceIdType.MESH
HEADS = 8
C = 256
T = 32
H = 16
F = 16
R = 16
PATCH = 8
BF = jnp.bfloat16
F32 = jnp.float32


def snake(i):
    half = i // 8
    return i + half * (23 - 2 * i)


def band_of(r):
    odd, x_low = (r // 4) % 2, (r // 2) % 2
    return r + odd * (2 - 4 * x_low)


def rms(x, gain):
    ms = jnp.mean(x * x, axis=-1, keepdims=True)
    return x * lax.rsqrt(ms + 1e-06) * gain


def silu(x):
    h = 0.5 * x
    return h + h * jnp.tanh(h)


def dot(a, b):
    return jnp.dot(a, b, preferred_element_type=F32)


def dot_tt(a, b, dims):
    return lax.dot_general(a, b, (dims, ((), ())), preferred_element_type=F32)


def inner_taps(act, kern, ys, h):
    slabs = [
        act[h, j : j + 2, l : l + PATCH].reshape(256, C) for j in range(3) for l in range(3)
    ]
    at = 8 + H * h
    for i in range(3):
        total = dot(slabs[0], kern[i * 9])
        for n in range(1, 9):
            total = total + dot(slabs[n], kern[i * 9 + n])
        ys[i, :, at : at + H] = total.reshape(16, H, C)


def edge_taps(north, south, west, east, kern, ys, h):
    rows = slice(8 + H * h, 8 + H * h + H)

    def chain(terms):
        total = None
        for lhs, tap in terms:
            term = dot(lhs.reshape(-1, C), kern[tap])
            total = term if total is None else total + term
        return total

    for i in range(3):
        top = chain([(north[h, l : l + PATCH], i * 9 + l) for l in range(3)])
        low = chain([(south[h, l : l + PATCH], i * 9 + 6 + l) for l in range(3)])
        left = chain([(west[h, j : j + 2], i * 9 + 3 * j) for j in range(3)])
        right = chain([(east[h, j : j + 2], i * 9 + 3 * j + 2) for j in range(3)])
        ys[i, 0:8, rows] += top.reshape(8, H, C)
        ys[i, 8:16, rows] += low.reshape(8, H, C)
        for row in range(2):
            ys[i, 8 * row, rows] += left[H * row : H * row + H]
            ys[i, 8 * row + 7, rows] += right[H * row : H * row + H]
    at = 8 + H * h
    total = ys[2, :, at : at + H] + ys[1, :, at - 1 : at - 1 + H] + ys[0, :, at - 2 : at - 2 + H]
    return total.reshape(256, C)


def iota(shape, dim):
    return lax.broadcasted_iota(jnp.int32, shape, dim)


def attend_row(h, row, qs, ks, vs, att, hmask, pmask):
    keys = H * (h + 1)
    group = 128 // keys
    scale = 32 ** -0.5 * 1.4426950408889634
    causal = iota((1, keys, 128), 1) <= (iota((1, keys, 128), 2) & 15) + H * h
    lane_head = iota((H, 128), 1) >> 5
    for u in range(row * 8 // group, (row + 1) * 8 // group):
        pixels = range(u * group, (u + 1) * group)
        scores = []
        for p in pixels:
            q_bd = jnp.concatenate([qs[h, p]] * 8, axis=0) * hmask[...]
            scores.append(dot_tt(ks[p, 0:keys], q_bd, ((1,), (1,))))
        s = jnp.concatenate(scores, axis=0).reshape(group, keys, 128)
        s = jnp.where(causal, s, -1e30)
        e = jnp.exp2((s - jnp.max(s, axis=1, keepdims=True)) * scale)
        probs = (e * (1.0 / jnp.sum(e, axis=1, keepdims=True))).astype(BF)
        probs = probs.reshape(128, 128).T
        value = vs[pl.ds(u * group, group), 0:keys].reshape(128, C)
        for hh in range(2):
            lanes = slice(128 * hh, 128 * hh + 128)
            part = value[:, lanes]
            v_bd = jnp.concatenate(
                [part * pmask[8 * h + n] for n in range(group)], axis=1)
            o = dot(probs[64 * hh : 64 * hh + 64], v_bd)
            for n, p in enumerate(pixels):
                tile = o[:, 128 * n : 128 * n + 128]
                got = tile[0:16]
                for k in range(1, 4):
                    got = jnp.where(lane_head == k, tile[16 * k : 16 * k + 16], got)
                att[p, :, lanes] = got.astype(BF)


def kernel(video, na, ca, nb, cb, nc, wq, wk, wv, wo, out,
           vloc, rin, xres, act_a, act_b, ka, kb, ga, gb, gc, sq, sk, sv, so,
           perm, perm_row, hmask, pmask, ya, yb, na_h, sa_h, wa_h, ea_h, nb_h, sb_h, wb_h, eb_h, qs, ks, vs, att, blk, sbuf,
           lsem, in_send, in_recv, ha_send, ha_recv, hb_send, hb_recv, out_send, out_recv):
    f = lax.axis_index("frames")
    r = lax.axis_index("rows")
    g = snake(f)
    mine = f // 8
    w = band_of(r)
    moved_band = (r // 4) % 2
    up, down = band_of((w + R - 1) % R), band_of((w + 1) % R)

    def remote(peer):
        return (peer != f) | (moved_band == 1)
    west, east = snake((g + F - 1) % F), snake((g + 1) % F)

    loads = [pltpu.make_async_copy(src, dst, lsem.at[n]) for n, (src, dst) in enumerate(
        [(video, vloc), (na, ga), (ca, ka), (nb, gb), (cb, kb), (nc, gc),
         (wq, sq), (wk, sk), (wv, sv), (wo, so)])]
    for load in loads:
        load.start()

    barrier = pltpu.get_barrier_semaphore()

    def greet(k, carry):
        @pl.when(remote(k))
        def _():
            pl.semaphore_signal(barrier, inc=1, device_id=(k, w), device_id_type=MESH)
        return carry

    lax.fori_loop(0, F, greet, 0)
    for ff in (west, east):
        pl.semaphore_signal(barrier, inc=1, device_id=(ff, r), device_id_type=MESH)
    for rr in (up, down):
        for ff in (west, f, east):
            pl.semaphore_signal(barrier, inc=1, device_id=(ff, rr), device_id_type=MESH)

    a, b = iota((256, 256), 0), iota((256, 256), 1)
    perm[...] = jnp.where(b == ((a & 15) << 4) + (a >> 4), 1.0, 0.0).astype(BF)
    hmask[...] = jnp.where(
        (iota((128, C), 0) >> 4) == (iota((128, C), 1) >> 5), 1.0, 0.0).astype(BF)
    a, b = iota((128, 128), 0), iota((128, 128), 1)
    perm_row[...] = jnp.where(b == ((a & 7) << 4) + (a >> 3), 1.0, 0.0).astype(BF)
    row_at = iota((128, 128), 0)
    for n in range(8):
        pmask[n] = jnp.where((row_at >> 4) == n, 1.0, 0.0).astype(BF)
    for n in range(4):
        pmask[8 + n] = jnp.where((row_at >> 5) == n, 1.0, 0.0).astype(BF)
    for ys in (ya, yb):
        ys[:, :, 0:8] = jnp.zeros((3, 16, 8, C), F32)
    for buf in (act_a, act_b):
        for at in (0, 3):
            buf[:, at] = jnp.zeros((2, PATCH + 2, H, C), BF)
        for at in (0, PATCH + 1):
            buf[:, 1:3, at] = jnp.zeros((2, 2, H, C), BF)
    for buf in (wa_h, ea_h, wb_h, eb_h):
        for at in (0, 3):
            buf[:, at] = jnp.zeros((2, H, C), BF)
    pl.semaphore_wait(barrier, F - 1 + moved_band + 8)
    loads[0].wait()

    def in_copy(k, peer, source):
        return pltpu.make_async_remote_copy(
            vloc.at[:, :, snake(peer)], rin.at[source], in_send.at[k], in_recv.at[source],
            device_id=(peer, w), device_id_type=MESH)

    def in_start(k, carry):
        peer = (f + k) % F

        @pl.when(remote(peer))
        def _():
            in_copy(k, peer, f).start()
        return carry

    lax.fori_loop(0, F, in_start, 0)

    @pl.when(moved_band == 0)
    def _():
        rin[f] = vloc[:, :, g]

    for load in loads[1:]:
        load.wait()


    def halo(buf, lands, send, recv, h):
        b = buf.at[h]
        north, south, west_h, east_h = (land.at[h] for land in lands)
        mid, two = pl.ds(1, PATCH), pl.ds(1, 2)
        plan = [
            (b.at[1, mid], south.at[mid], (f, up)),
            (b.at[2, mid], north.at[mid], (f, down)),
            (b.at[1, 1], south.at[PATCH + 1], (west, up)),
            (b.at[1, PATCH], south.at[0], (east, up)),
            (b.at[2, 1], north.at[PATCH + 1], (west, down)),
            (b.at[2, PATCH], north.at[0], (east, down)),
            (b.at[two, 1], east_h.at[two], (west, r)),
            (b.at[two, PATCH], west_h.at[two], (east, r)),
        ]
        copies = [
            pltpu.make_async_remote_copy(
                src, dst, send.at[8 * h + n], recv.at[8 * h + n],
                device_id=to, device_id_type=MESH)
            for n, (src, dst, to) in enumerate(plan)
        ]
        return copies

    def halo_start(copies, before=()):
        for copy in before:
            copy.wait_send()
        for copy in copies:
            copy.start()

    def halo_end(lands, copies, h):
        for copy in copies:
            copy.wait_recv()
        north, south, west_h, east_h = lands

        @pl.when(w == 0)
        def _():
            north[h] = jnp.zeros((PATCH + 2, H, C), BF)

        @pl.when(w == R - 1)
        def _():
            south[h] = jnp.zeros((PATCH + 2, H, C), BF)

        @pl.when(g == 0)
        def _():
            north[h, 0] = jnp.zeros((H, C), BF)
            south[h, 0] = jnp.zeros((H, C), BF)
            west_h[h, 1:3] = jnp.zeros((2, H, C), BF)

        @pl.when(g == F - 1)
        def _():
            north[h, PATCH + 1] = jnp.zeros((H, C), BF)
            south[h, PATCH + 1] = jnp.zeros((H, C), BF)
            east_h[h, 1:3] = jnp.zeros((2, H, C), BF)

    lands_a = (na_h, sa_h, wa_h, ea_h)
    lands_b = (nb_h, sb_h, wb_h, eb_h)
    halos_a, halos_b = [], []
    for h in range(2):
        def in_wait(k, carry):
            src = 8 * h + k

            @pl.when(remote(src))
            def _():
                in_copy(0, src, src).wait_recv()
            return carry

        lax.fori_loop(0, 8, in_wait, 0)
        x = dot(perm[...], rin[8 * h : 8 * h + 8].reshape(256, C))
        xres[h] = x.astype(BF)
        act = silu(rms(x, ga[...])).astype(BF)
        act_a[h, 1:3, 1 : PATCH + 1] = act.reshape(2, PATCH, H, C)
        halos_a.append(halo(act_a, lands_a, ha_send, ha_recv, h))
        if h == 0:
            halo_start(halos_a[0])

    inner_taps(act_a, ka, ya, 0)
    halo_start(halos_a[1], halos_a[0])
    inner_taps(act_a, ka, ya, 1)
    for h in range(2):
        halo_end(lands_a, halos_a[h], h)
        inner = edge_taps(*lands_a, ka, ya, h).astype(BF).astype(F32)
        act = silu(rms(inner, gb[...])).astype(BF)
        act_b[h, 1:3, 1 : PATCH + 1] = act.reshape(2, PATCH, H, C)
        halos_b.append(halo(act_b, lands_b, hb_send, hb_recv, h))
        halo_start(halos_b[h], halos_b[0] if h else halos_a[1])
    for h in range(2):
        inner_taps(act_b, kb, yb, h)

    def out_copy(dst, source, row, k):
        return pltpu.make_async_remote_copy(
            sbuf.at[dst, row], out.at[:, row, snake(source)],
            out_send.at[2 * k + row], out_recv.at[2 * source + row],
            device_id=(dst, w), device_id_type=MESH)

    own = [pltpu.make_async_copy(sbuf.at[f, row], out.at[:, row, g], lsem.at[row])
           for row in range(2)]
    for h in range(2):
        halo_end(lands_b, halos_b[h], h)
        block = (xres[h].astype(F32) + edge_taps(*lands_b, kb, yb, h)).astype(BF)
        blk[...] = block
        normed = rms(block.astype(F32), gc[...]).astype(BF)
        qs[h] = dot(normed, sq[...]).astype(BF).reshape(16, H, C)
        ks[:, H * h : H * h + H] = dot(normed, sk[...]).astype(BF).reshape(16, H, C)
        vs[:, H * h : H * h + H] = dot(normed, sv[...]).astype(BF).reshape(16, H, C)
        for row in range(2 if h == 0 else 0):
            attend_row(h, row, qs, ks, vs, att, hmask, pmask)
        for row in range(2):
            if h == 1:
                attend_row(h, row, qs, ks, vs, att, hmask, pmask)
            at = slice(128 * row, 128 * row + 128)
            projected = dot(att[8 * row : 8 * row + 8].reshape(128, C), so[...])
            encoded = (blk[at].astype(F32) + projected.astype(BF).astype(F32)).astype(BF)
            moved = dot(perm_row[...], encoded).astype(BF)
            sbuf[8 * h : 8 * h + 8, row] = moved.reshape(8, 2, PATCH, C)

            @pl.when((mine == h) & (moved_band == 0))
            def _():
                own[row].start()

            def out_start(k, carry):
                dst = 8 * h + k

                @pl.when(remote(dst))
                def _():
                    out_copy(dst, f, row, dst).start()
                return carry

            lax.fori_loop(0, 8, out_start, 0)

    def finish(k, carry):
        src = (f + k) % F

        @pl.when(remote(src))
        def _():
            in_copy(k, src, src).wait_send()
            for row in range(2):
                out_copy(src, src, row, src).wait()
        return carry

    lax.fori_loop(0, F, finish, 0)
    for copy in halos_b[1]:
        copy.wait_send()

    @pl.when(moved_band == 0)
    def _():
        for copy in own:
            copy.wait()


def shards(video, na, ca, nb, cb, nc, wq, wk, wv, wo):
    any_spec = pl.BlockSpec(memory_space=pltpu.HBM)
    dma = pltpu.SemaphoreType.DMA
    vm = pltpu.VMEM
    halo = (2, 4, PATCH + 2, H, C)
    lands = [vm((2, n, H, C), BF) for n in (PATCH + 2, PATCH + 2, 4, 4)]
    out = pl.pallas_call(
        kernel,
        out_shape=pltpu.VMEM((2, 2, F, PATCH, C), BF),
        in_specs=[any_spec] * 10,
        out_specs=pl.BlockSpec(memory_space=pltpu.VMEM),
        scratch_shapes=[
            vm((2, 2, F, PATCH, C), BF), vm((F, 2, 2, PATCH, C), BF), vm((2, 256, C), BF),
            vm(halo, BF), vm(halo, BF), vm((27, C, C), BF), vm((27, C, C), BF),
            vm((1, C), F32), vm((1, C), F32), vm((1, C), F32),
            vm((C, C), BF), vm((C, C), BF), vm((C, C), BF), vm((C, C), BF),
            vm((256, 256), BF), vm((128, 128), BF), vm((128, C), BF), vm((12, 128, 128), BF),
            vm((3, 16, 40, C), F32), vm((3, 16, 40, C), F32),
            *lands, *lands,
            vm((2, 16, H, C), BF), vm((16, T, C), BF), vm((16, T, C), BF), vm((16, H, C), BF),
            vm((256, C), BF), vm((F, 2, 2, PATCH, C), BF),
            dma((10,)), dma((F,)), dma((F,)), dma((16,)), dma((16,)), dma((16,)), dma((16,)),
            dma((2 * F,)), dma((2 * F,)),
        ],
        compiler_params=pltpu.CompilerParams(
            collective_id=0, has_side_effects=True, vmem_limit_bytes=60 * 1024 * 1024),
    )(
        video.reshape(2, 2, F, PATCH, C), na.reshape(1, C), ca.reshape(27, C, C), nb.reshape(1, C),
        cb.reshape(27, C, C), nc.reshape(1, C), wq, wk, wv, wo,
    )
    return out.reshape(2, 2, F * PATCH, C)


def solution(mesh):
    placed = (P("frames", "rows", None, None), P(), P(), P(), P(), P(), P(), P(), P(), P())
    return jax.shard_map(
        shards,
        mesh=mesh,
        in_specs=placed,
        out_specs=P("frames", "rows", None, None),
        check_vma=False,
    )
```

```python
import functools

import jax
import jax.numpy as jnp
from jax import lax
from jax.experimental import pallas as pl
from jax.experimental.pallas import tpu as pltpu
from jax.sharding import PartitionSpec as P

MESH = pl.DeviceIdType.MESH
HEADS = 8
C = 256
T = 32
H = 16
F = 16
R = 16
PATCH = 8
BF = jnp.bfloat16
F32 = jnp.float32


def snake(i):
    half = i // 8
    return i + half * (23 - 2 * i)


def band_of(r):
    odd, x_low = (r // 4) % 2, (r // 2) % 2
    return r + odd * (2 - 4 * x_low)


def rms(x, gain):
    ms = jnp.mean(x * x, axis=-1, keepdims=True)
    return x * lax.rsqrt(ms + 1e-06) * gain


def silu(x):
    h = 0.5 * x
    return h + h * jnp.tanh(h)


def dot(a, b):
    return jnp.dot(a, b, preferred_element_type=F32)


def dot_tt(a, b, dims):
    return lax.dot_general(a, b, (dims, ((), ())), preferred_element_type=F32)


def inner_taps(act, kern, ys, h):
    slabs = [
        act[h, j : j + 2, l : l + PATCH].reshape(256, C) for j in range(3) for l in range(3)
    ]
    at = 8 + H * h
    for i in range(3):
        total = dot(slabs[0], kern[i * 9])
        for n in range(1, 9):
            total = total + dot(slabs[n], kern[i * 9 + n])
        ys[i, :, at : at + H] = total.reshape(16, H, C)


def edge_taps(north, south, west, east, kern, ys, h):
    rows = slice(8 + H * h, 8 + H * h + H)

    def chain(terms):
        total = None
        for lhs, tap in terms:
            term = dot(lhs.reshape(-1, C), kern[tap])
            total = term if total is None else total + term
        return total

    for i in range(3):
        top = chain([(north[h, l : l + PATCH], i * 9 + l) for l in range(3)])
        low = chain([(south[h, l : l + PATCH], i * 9 + 6 + l) for l in range(3)])
        left = chain([(west[h, j : j + 2], i * 9 + 3 * j) for j in range(3)])
        right = chain([(east[h, j : j + 2], i * 9 + 3 * j + 2) for j in range(3)])
        ys[i, 0:8, rows] += top.reshape(8, H, C)
        ys[i, 8:16, rows] += low.reshape(8, H, C)
        for row in range(2):
            ys[i, 8 * row, rows] += left[H * row : H * row + H]
            ys[i, 8 * row + 7, rows] += right[H * row : H * row + H]
    at = 8 + H * h
    total = ys[2, :, at : at + H] + ys[1, :, at - 1 : at - 1 + H] + ys[0, :, at - 2 : at - 2 + H]
    return total.reshape(256, C)


def iota(shape, dim):
    return lax.broadcasted_iota(jnp.int32, shape, dim)


def attend_row(h, row, qs, ks, vs, att, hmask, pmask):
    keys = H * (h + 1)
    group = 128 // keys
    scale = 32 ** -0.5 * 1.4426950408889634
    causal = iota((1, keys, 128), 1) <= (iota((1, keys, 128), 2) & 15) + H * h
    lane_head = iota((H, 128), 1) >> 5
    for u in range(row * 8 // group, (row + 1) * 8 // group):
        pixels = range(u * group, (u + 1) * group)
        scores = []
        for p in pixels:
            q_bd = jnp.concatenate([qs[h, p]] * 8, axis=0) * hmask[...]
            scores.append(dot_tt(ks[p, 0:keys], q_bd, ((1,), (1,))))
        s = jnp.concatenate(scores, axis=0).reshape(group, keys, 128)
        s = jnp.where(causal, s, -1e30)
        e = jnp.exp2((s - jnp.max(s, axis=1, keepdims=True)) * scale)
        probs = (e * (1.0 / jnp.sum(e, axis=1, keepdims=True))).astype(BF)
        probs = probs.reshape(128, 128).T
        value = vs[pl.ds(u * group, group), 0:keys].reshape(128, C)
        for hh in range(2):
            lanes = slice(128 * hh, 128 * hh + 128)
            part = value[:, lanes]
            v_bd = jnp.concatenate(
                [part * pmask[8 * h + n] for n in range(group)], axis=1)
            o = dot(probs[64 * hh : 64 * hh + 64], v_bd)
            for n, p in enumerate(pixels):
                tile = o[:, 128 * n : 128 * n + 128]
                got = tile[0:16]
                for k in range(1, 4):
                    got = jnp.where(lane_head == k, tile[16 * k : 16 * k + 16], got)
                att[p, :, lanes] = got.astype(BF)


def kernel(video, na, ca, nb, cb, nc, wq, wk, wv, wo, out,
           vloc, rin, xres, act_a, act_b, ka, kb, ga, gb, gc, sq, sk, sv, so,
           perm, perm_row, hmask, pmask, ya, yb, na_h, sa_h, wa_h, ea_h, nb_h, sb_h, wb_h, eb_h, qs, ks, vs, att, blk, sbuf,
           lsem, in_send, in_recv, ha_send, ha_recv, hb_send, hb_recv, out_send, out_recv):
    f = lax.axis_index("frames")
    r = lax.axis_index("rows")
    g = snake(f)
    mine = f // 8
    w = band_of(r)
    moved_band = (r // 4) % 2
    up, down = band_of((w + R - 1) % R), band_of((w + 1) % R)

    def remote(peer):
        return (peer != f) | (moved_band == 1)
    west, east = snake((g + F - 1) % F), snake((g + 1) % F)

    barrier = pltpu.get_barrier_semaphore()

    def greet(k, carry):
        peer = (f + 4 + k) % F

        @pl.when(remote(peer))
        def _():
            pl.semaphore_signal(barrier, inc=1, device_id=(peer, w), device_id_type=MESH)
        return carry

    lax.fori_loop(0, F, greet, 0)
    for ff in (west, east):
        pl.semaphore_signal(barrier, inc=1, device_id=(ff, r), device_id_type=MESH)
    for rr in (up, down):
        for ff in (west, f, east):
            pl.semaphore_signal(barrier, inc=1, device_id=(ff, rr), device_id_type=MESH)

    loads = [pltpu.make_async_copy(src, dst, lsem.at[n]) for n, (src, dst) in enumerate(
        [(video, vloc), (na, ga), (ca, ka), (nb, gb), (cb, kb), (nc, gc),
         (wq, sq), (wk, sk), (wv, sv), (wo, so)])]
    for load in loads:
        load.start()

    a, b = iota((256, 256), 0), iota((256, 256), 1)
    perm[...] = jnp.where(b == ((a & 15) << 4) + (a >> 4), 1.0, 0.0).astype(BF)
    hmask[...] = jnp.where(
        (iota((128, C), 0) >> 4) == (iota((128, C), 1) >> 5), 1.0, 0.0).astype(BF)
    a, b = iota((128, 128), 0), iota((128, 128), 1)
    perm_row[...] = jnp.where(b == ((a & 7) << 4) + (a >> 3), 1.0, 0.0).astype(BF)
    row_at = iota((128, 128), 0)
    for n in range(8):
        pmask[n] = jnp.where((row_at >> 4) == n, 1.0, 0.0).astype(BF)
    for n in range(4):
        pmask[8 + n] = jnp.where((row_at >> 5) == n, 1.0, 0.0).astype(BF)
    for ys in (ya, yb):
        ys[:, :, 0:8] = jnp.zeros((3, 16, 8, C), F32)
    for buf in (act_a, act_b):
        for at in (0, 3):
            buf[:, at] = jnp.zeros((2, PATCH + 2, H, C), BF)
        for at in (0, PATCH + 1):
            buf[:, 1:3, at] = jnp.zeros((2, 2, H, C), BF)
    for buf in (wa_h, ea_h, wb_h, eb_h):
        for at in (0, 3):
            buf[:, at] = jnp.zeros((2, H, C), BF)
    pl.semaphore_wait(barrier, F - 1 + moved_band + 8)
    loads[0].wait()

    def in_copy(k, peer, source):
        return pltpu.make_async_remote_copy(
            vloc.at[:, :, snake(peer)], rin.at[source], in_send.at[k], in_recv.at[source],
            device_id=(peer, w), device_id_type=MESH)

    def in_start(k, carry):
        peer = (f + k) % F

        @pl.when(remote(peer))
        def _():
            in_copy(k, peer, f).start()
        return carry

    lax.fori_loop(0, F, in_start, 0)

    @pl.when(moved_band == 0)
    def _():
        rin[f] = vloc[:, :, g]

    for load in loads[1:]:
        load.wait()


    def halo(buf, lands, send, recv, h):
        b = buf.at[h]
        north, south, west_h, east_h = (land.at[h] for land in lands)
        mid, two = pl.ds(1, PATCH), pl.ds(1, 2)
        plan = [
            (b.at[1, mid], south.at[mid], (f, up)),
            (b.at[2, mid], north.at[mid], (f, down)),
            (b.at[1, 1], south.at[PATCH + 1], (west, up)),
            (b.at[1, PATCH], south.at[0], (east, up)),
            (b.at[2, 1], north.at[PATCH + 1], (west, down)),
            (b.at[2, PATCH], north.at[0], (east, down)),
            (b.at[two, 1], east_h.at[two], (west, r)),
            (b.at[two, PATCH], west_h.at[two], (east, r)),
        ]
        copies = [
            pltpu.make_async_remote_copy(
                src, dst, send.at[8 * h + n], recv.at[8 * h + n],
                device_id=to, device_id_type=MESH)
            for n, (src, dst, to) in enumerate(plan)
        ]
        return copies

    def halo_start(copies, before=()):
        for copy in before:
            copy.wait_send()
        for copy in copies:
            copy.start()

    def halo_end(lands, copies, h):
        for copy in copies:
            copy.wait_recv()
        north, south, west_h, east_h = lands

        @pl.when(w == 0)
        def _():
            north[h] = jnp.zeros((PATCH + 2, H, C), BF)

        @pl.when(w == R - 1)
        def _():
            south[h] = jnp.zeros((PATCH + 2, H, C), BF)

        @pl.when(g == 0)
        def _():
            north[h, 0] = jnp.zeros((H, C), BF)
            south[h, 0] = jnp.zeros((H, C), BF)
            west_h[h, 1:3] = jnp.zeros((2, H, C), BF)

        @pl.when(g == F - 1)
        def _():
            north[h, PATCH + 1] = jnp.zeros((H, C), BF)
            south[h, PATCH + 1] = jnp.zeros((H, C), BF)
            east_h[h, 1:3] = jnp.zeros((2, H, C), BF)

    lands_a = (na_h, sa_h, wa_h, ea_h)
    lands_b = (nb_h, sb_h, wb_h, eb_h)
    halos_a, halos_b = [], []
    for h in range(2):
        def in_wait(k, carry):
            src = 8 * h + k

            @pl.when(remote(src))
            def _():
                in_copy(0, src, src).wait_recv()
            return carry

        lax.fori_loop(0, 8, in_wait, 0)
        x = dot(perm[...], rin[8 * h : 8 * h + 8].reshape(256, C))
        xres[h] = x.astype(BF)
        act = silu(rms(x, ga[...])).astype(BF)
        act_a[h, 1:3, 1 : PATCH + 1] = act.reshape(2, PATCH, H, C)
        halos_a.append(halo(act_a, lands_a, ha_send, ha_recv, h))
        if h == 0:
            halo_start(halos_a[0])

    inner_taps(act_a, ka, ya, 0)
    halo_start(halos_a[1], halos_a[0])
    inner_taps(act_a, ka, ya, 1)
    for h in range(2):
        halo_end(lands_a, halos_a[h], h)
        inner = edge_taps(*lands_a, ka, ya, h).astype(BF).astype(F32)
        act = silu(rms(inner, gb[...])).astype(BF)
        act_b[h, 1:3, 1 : PATCH + 1] = act.reshape(2, PATCH, H, C)
        halos_b.append(halo(act_b, lands_b, hb_send, hb_recv, h))
        halo_start(halos_b[h], halos_b[0] if h else halos_a[1])
    for h in range(2):
        inner_taps(act_b, kb, yb, h)

    def out_copy(dst, source, row, k):
        return pltpu.make_async_remote_copy(
            sbuf.at[dst, row], out.at[:, row, snake(source)],
            out_send.at[2 * k + row], out_recv.at[2 * source + row],
            device_id=(dst, w), device_id_type=MESH)

    own = [pltpu.make_async_copy(sbuf.at[f, row], out.at[:, row, g], lsem.at[row])
           for row in range(2)]
    for h in range(2):
        halo_end(lands_b, halos_b[h], h)
        block = (xres[h].astype(F32) + edge_taps(*lands_b, kb, yb, h)).astype(BF)
        blk[...] = block
        normed = rms(block.astype(F32), gc[...]).astype(BF)
        qs[h] = dot(normed, sq[...]).astype(BF).reshape(16, H, C)
        ks[:, H * h : H * h + H] = dot(normed, sk[...]).astype(BF).reshape(16, H, C)
        vs[:, H * h : H * h + H] = dot(normed, sv[...]).astype(BF).reshape(16, H, C)
        for row in range(2 if h == 0 else 0):
            attend_row(h, row, qs, ks, vs, att, hmask, pmask)
        for row in range(2):
            if h == 1:
                attend_row(h, row, qs, ks, vs, att, hmask, pmask)
            at = slice(128 * row, 128 * row + 128)
            projected = dot(att[8 * row : 8 * row + 8].reshape(128, C), so[...])
            encoded = (blk[at].astype(F32) + projected.astype(BF).astype(F32)).astype(BF)
            moved = dot(perm_row[...], encoded).astype(BF)
            sbuf[8 * h : 8 * h + 8, row] = moved.reshape(8, 2, PATCH, C)

            @pl.when((mine == h) & (moved_band == 0))
            def _():
                own[row].start()

            def out_start(k, carry):
                dst = 8 * h + k

                @pl.when(remote(dst))
                def _():
                    out_copy(dst, f, row, dst).start()
                return carry

            lax.fori_loop(0, 8, out_start, 0)

    def finish(k, carry):
        src = (f + k) % F

        @pl.when(remote(src))
        def _():
            in_copy(k, src, src).wait_send()
            for row in range(2):
                out_copy(src, src, row, src).wait()
        return carry

    lax.fori_loop(0, F, finish, 0)
    for copy in halos_b[1]:
        copy.wait_send()

    @pl.when(moved_band == 0)
    def _():
        for copy in own:
            copy.wait()


def shards(video, na, ca, nb, cb, nc, wq, wk, wv, wo):
    any_spec = pl.BlockSpec(memory_space=pltpu.HBM)
    dma = pltpu.SemaphoreType.DMA
    vm = pltpu.VMEM
    halo = (2, 4, PATCH + 2, H, C)
    lands = [vm((2, n, H, C), BF) for n in (PATCH + 2, PATCH + 2, 4, 4)]
    out = pl.pallas_call(
        kernel,
        out_shape=pltpu.VMEM((2, 2, F, PATCH, C), BF),
        in_specs=[any_spec] * 10,
        out_specs=pl.BlockSpec(memory_space=pltpu.VMEM),
        scratch_shapes=[
            vm((2, 2, F, PATCH, C), BF), vm((F, 2, 2, PATCH, C), BF), vm((2, 256, C), BF),
            vm(halo, BF), vm(halo, BF), vm((27, C, C), BF), vm((27, C, C), BF),
            vm((1, C), F32), vm((1, C), F32), vm((1, C), F32),
            vm((C, C), BF), vm((C, C), BF), vm((C, C), BF), vm((C, C), BF),
            vm((256, 256), BF), vm((128, 128), BF), vm((128, C), BF), vm((12, 128, 128), BF),
            vm((3, 16, 40, C), F32), vm((3, 16, 40, C), F32),
            *lands, *lands,
            vm((2, 16, H, C), BF), vm((16, T, C), BF), vm((16, T, C), BF), vm((16, H, C), BF),
            vm((256, C), BF), vm((F, 2, 2, PATCH, C), BF),
            dma((10,)), dma((F,)), dma((F,)), dma((16,)), dma((16,)), dma((16,)), dma((16,)),
            dma((2 * F,)), dma((2 * F,)),
        ],
        compiler_params=pltpu.CompilerParams(
            collective_id=0, has_side_effects=True, vmem_limit_bytes=60 * 1024 * 1024),
    )(
        video.reshape(2, 2, F, PATCH, C), na.reshape(1, C), ca.reshape(27, C, C), nb.reshape(1, C),
        cb.reshape(27, C, C), nc.reshape(1, C), wq, wk, wv, wo,
    )
    return out.reshape(2, 2, F * PATCH, C)


def solution(mesh):
    placed = (P("frames", "rows", None, None), P(), P(), P(), P(), P(), P(), P(), P(), P())
    return jax.shard_map(
        shards,
        mesh=mesh,
        in_specs=placed,
        out_specs=P("frames", "rows", None, None),
        check_vma=False,
    )
```
